128 devices in a mesh: section: 2 (over x_hi), dp: 16 (over z, y), mp: 4 (over x_lo, core).
Axes of the slice: x: 4 (x_hi: 2, x_lo: 2; x = x_hi * 2 + x_lo), y: 4, z: 4, core: 2. Of those that a mesh axis runs over, the one named last changes fastest.
Arguments:
- text_feats: bfloat16 [16384, 512], P('dp'), may hold values from -48 to 48
- image_feats: bfloat16 [16384, 512], P(('dp', 'mp')), may hold values from -48 to 48
- logit_scale: float32 [1], replicated, may hold values from 10 to 320
- layer_inputs: bfloat16 [2, 16384, 512], P('section', 'dp'), may hold values from -6 to 6
- w_in: bfloat16 [2, 512, 2048], P('section', None, 'mp'), may hold values from -0.25 to 0.25
- w_out: bfloat16 [2, 2048, 512], P('section', 'mp'), may hold values from -0.125 to 0.125
Outputs:
- image_grad: bfloat16 [16384, 512], P(('dp', 'mp'))
- input_grad: bfloat16 [16384, 512], P('dp', 'section')
- w_in_grad: float32 [2, 512, 2048], P('section', 'dp', 'mp')
- w_out_grad_t: float32 [2, 512, 2048], P('section', 'dp', 'mp')
The draws below stay inside these ranges and needn't reach their ends.
All inputs are finite; a program needn't handle non-finite values.
Results may differ from the reference program's by a relative error of at most 0.017.
Values may be sent and summed in bfloat16 or wider, within the bound.
No kernel may reach another device: no remote copies, remote signals or barrier semaphores. Data moves between devices by JAX's collectives and lax.ppermute only.
A program may use at most 128 MiB of HBM per device.

```python
import jax
import jax.numpy as jnp
from jax import lax

D = 512
FF = 2048
PAIRS_DEV = 1024
PAIRS = 16384
LAYERS = 2


def joint_feats(key):
    folded = jax.random.fold_in(key, 11)
    key_shared, key_text, key_image, key_scale = jax.random.split(folded, 4)
    shared = jnp.clip(jax.random.normal(key_shared, (PAIRS, D), jnp.float32), -4.0, 4.0)
    text_noise = jnp.clip(jax.random.normal(key_text, (PAIRS, D), jnp.float32), -4.0, 4.0)
    image_noise = jnp.clip(jax.random.normal(key_image, (PAIRS, D), jnp.float32), -4.0, 4.0)
    text_rows = shared + text_noise
    image_rows = shared + image_noise
    return (text_rows, image_rows)


def draw_text_feats(key, part):
    text_rows, image_rows = joint_feats(key)
    return text_rows.astype(jnp.bfloat16)


def draw_image_feats(key, part):
    text_rows, image_rows = joint_feats(key)
    return image_rows.astype(jnp.bfloat16)


def draw_logit_scale(key, part):
    folded = jax.random.fold_in(key, 23)
    return jax.random.uniform(folded, (1,), jnp.float32, 10.0, 30.0)


def block_levels(rng, dims, cuts, smallest, top_value):
    factor_of, own = 1.0, jax.random.fold_in(rng, 6)
    for dim, parts in cuts:
        steps = jnp.exp(jax.random.uniform(jax.random.fold_in(own, dim), (parts,), jnp.float32, smallest / len(cuts), top_value / len(cuts)))
        factor_of = factor_of * jnp.repeat(steps, dims[dim] // parts).reshape([-1 if axis == dim else 1 for axis in range(len(dims))])
    return factor_of


def gaussian(key, extent, deviation, limit, cuts=(), kind=jnp.bfloat16):
    entries = jax.random.normal(key, extent, jnp.float32) * deviation
    if len(cuts) > 0:
        entries = block_levels(key, extent, cuts, -0.22, 0.18) * entries
    return jnp.clip(entries, min=-limit, max=limit).astype(kind)


def setup_inputs(seed: int = 0) -> dict:
    splits = jax.random.split(jax.random.key(seed), 7)
    text_feats = draw_text_feats(jax.random.fold_in(splits[6], 71), 0)
    image_feats = draw_image_feats(jax.random.fold_in(splits[6], 71), 0)
    logit_scale = draw_logit_scale(jax.random.fold_in(splits[6], 71), 0)
    layer_inputs = gaussian(splits[3], (LAYERS, PAIRS, D), 1.0, 6.0, ((0, 2), (1, 16)))
    w_in = gaussian(splits[4], (LAYERS, D, FF), D ** -0.5, 0.25, ((0, 2), (2, 4)))
    w_out = gaussian(splits[5], (LAYERS, FF, D), FF ** -0.5, 0.125, ((0, 2), (1, 4)))
    return {"text_feats": text_feats, "image_feats": image_feats, "logit_scale": logit_scale, "layer_inputs": layer_inputs, "w_in": w_in, "w_out": w_out}


def unit_rows(values):
    wide = values.astype(jnp.float32)
    length = jnp.sqrt(lax.optimization_barrier(jnp.sum(wide * wide, axis=1, keepdims=True)) + 1.0)
    return (wide / length, length)

def unit_backward(unit, length, grad_unit):
    return (grad_unit - unit * lax.optimization_barrier(jnp.sum(unit * grad_unit, axis=1, keepdims=True))) / length

def quick_gelu(values):
    return values * jax.nn.sigmoid(1.702 * values)

def quick_slope(values):
    sigm = jax.nn.sigmoid(1.702 * values)
    return sigm + 1.702 * values * sigm * (1.0 - sigm)

def reference(text_feats, image_feats, logit_scale, layer_inputs, w_in, w_out):
    logit_mult = logit_scale[0]
    text_unit, text_length = unit_rows(text_feats)
    image_unit, image_length = unit_rows(image_feats)
    text_low = text_unit.astype(jnp.bfloat16)
    image_low = image_unit.astype(jnp.bfloat16)
    block_count = PAIRS // PAIRS_DEV
    text_blocks = text_low.reshape(block_count, PAIRS_DEV, D)
    block_ids = jnp.arange(block_count, dtype=jnp.int32)
    column_ids = jnp.arange(PAIRS, dtype=jnp.int32)

    def stats_step(state_pair, text_block):
        column_peak, column_total = state_pair
        scores = logit_mult * jnp.dot(text_block, image_low.T, preferred_element_type=jnp.float32)
        row_peak = lax.optimization_barrier(jnp.max(scores, axis=1))
        row_total = lax.optimization_barrier(jnp.sum(jnp.exp(scores - row_peak[:, None]), axis=1))
        new_peak = jnp.maximum(column_peak, lax.optimization_barrier(jnp.max(scores, axis=0)))
        column_total = column_total * jnp.exp(column_peak - new_peak) + lax.optimization_barrier(jnp.sum(jnp.exp(scores - new_peak[None, :]), axis=0))
        return ((new_peak, column_total), (row_peak, row_total))
    start_pair = (jnp.full((PAIRS,), -1e+30, jnp.float32), jnp.zeros((PAIRS,), jnp.float32))
    (column_peak, column_total), (row_peaks, row_totals) = lax.scan(stats_step, start_pair, text_blocks)

    def grad_step(image_acc, inputs):
        text_block, row_peak, row_total, block_id = inputs
        scores = logit_mult * jnp.dot(text_block, image_low.T, preferred_element_type=jnp.float32)
        text_ids = (block_id * PAIRS_DEV + jnp.arange(PAIRS_DEV, dtype=jnp.int32)).astype(jnp.int32)
        positive = (text_ids[:, None] == column_ids[None, :]).astype(jnp.float32)
        row_prob = jnp.exp(scores - row_peak[:, None]) / row_total[:, None]
        column_prob = jnp.exp(scores - column_peak[None, :]) / column_total[None, :]
        score_grad = (0.5 * (row_prob + column_prob) - positive).astype(jnp.bfloat16)
        text_part = logit_mult * jnp.dot(score_grad, image_low, preferred_element_type=jnp.float32)
        image_acc = image_acc + logit_mult * jnp.dot(score_grad.T, text_block, preferred_element_type=jnp.float32)
        return (image_acc, text_part)
    image_unit_grad, text_parts = lax.scan(grad_step, jnp.zeros((PAIRS, D), jnp.float32), (text_blocks, row_peaks, row_totals, block_ids))
    text_unit_grad = text_parts.reshape(PAIRS, D)
    top_grad = unit_backward(text_unit, text_length, text_unit_grad).astype(jnp.bfloat16)
    image_grad = unit_backward(image_unit, image_length, image_unit_grad).astype(jnp.bfloat16)
    layer_grad = top_grad
    first_grads = []
    second_grads = []
    for layer in reversed(range(LAYERS)):
        inputs_now = layer_inputs[layer]
        pre_act = jnp.dot(inputs_now, w_in[layer], preferred_element_type=jnp.float32)
        activation = quick_gelu(pre_act).astype(jnp.bfloat16)
        back_grad = jnp.dot(layer_grad, w_out[layer].T, preferred_element_type=jnp.float32)
        pre_grad = (back_grad * quick_slope(pre_act)).astype(jnp.bfloat16)
        first_grads.insert(0, jnp.dot(inputs_now.T, pre_grad, preferred_element_type=jnp.float32))
        second_grads.insert(0, jnp.dot(layer_grad.T, activation, preferred_element_type=jnp.float32))
        layer_grad = (layer_grad.astype(jnp.float32) + jnp.dot(pre_grad, w_in[layer].T, preferred_element_type=jnp.float32)).astype(jnp.bfloat16)
    return (image_grad, layer_grad, jnp.stack(first_grads), jnp.stack(second_grads))
```

```python
import functools

import jax
import jax.numpy as jnp
from jax import lax
from jax.experimental import pallas as pl
from jax.experimental.pallas import tpu as pltpu
from jax.sharding import PartitionSpec as P


BF = jnp.bfloat16
F32 = jnp.float32
LOG2E = 1.4426950408889634
GROUP = ("section", "mp")


def unit_rows(values):
    wide = values.astype(F32)
    length = jnp.sqrt(jnp.sum(wide * wide, axis=1, keepdims=True) + 1.0)
    return (wide / length, length)


def unit_backward(unit, length, grad_unit):
    return (grad_unit - unit * jnp.sum(unit * grad_unit, axis=1, keepdims=True)) / length


def torus_shift(value, dz, dy):
    route = [
        (z * 4 + y, ((z + dz) % 4) * 4 + (y + dy) % 4) for z in range(4) for y in range(4)
    ]
    return lax.ppermute(value, "dp", route)


def chip_swap(value, k):
    return lax.ppermute(value, GROUP, [(i, i ^ (2 * k)) for i in range(8)])


def core_swap(value):
    return lax.ppermute(value, GROUP, [(i, i ^ 1) for i in range(8)])


def dot_rows(a, b):
    return lax.dot_general(a, b, (((0,), (0,)), ((), ())), preferred_element_type=F32)


def dot_cols(a, b):
    return lax.dot_general(a, b, (((1,), (1,)), ((), ())), preferred_element_type=F32)


def dot(a, b):
    return jnp.dot(a, b, preferred_element_type=F32)


def to_lanes(column):
    rows = column.shape[0]
    return jnp.broadcast_to(column, (rows, 128)).T[0:1, :]


def to_sublanes(row):
    return jnp.broadcast_to(row, (128, row.shape[1])).T[:, 0:1]


def assemble(parts, target):
    for colour in range(2):
        for k in range(4):
            for j in range(4):
                zr, yr = (k, j) if colour == 0 else (j, k)
                at = (zr * 4 + yr) * 128 + colour * 64
                target[at : at + 64, :] = parts[colour * 4 + k][j * 64 : j * 64 + 64, :]


def score_kernel(scale_ref, text_ref, *refs):
    parts, (s_ref, row_ref, col_ref, image) = refs[:8], refs[8:]
    step = pl.program_id(0)

    @pl.when(step == 0)
    def _():
        assemble(parts, image)

    s = dot_cols(text_ref[...], image[...]) * (scale_ref[0] * LOG2E)
    s_ref[...] = s
    row_max = jnp.max(s, axis=1, keepdims=True)
    row_sum = jnp.sum(jnp.exp2(s - row_max), axis=1, keepdims=True)
    row_ref[0:1, :] = to_lanes(row_max)
    row_ref[1:2, :] = to_lanes(row_sum)
    peak = jnp.max(s, axis=0, keepdims=True)

    @pl.when(step == 0)
    def _():
        col_ref[0:1, :] = peak
        col_ref[1:2, :] = jnp.sum(jnp.exp2(s - peak), axis=0, keepdims=True)

    @pl.when(step > 0)
    def _():
        old = col_ref[0:1, :]
        new = jnp.maximum(old, peak)
        col_ref[0:1, :] = new
        col_ref[1:2, :] = col_ref[1:2, :] * jnp.exp2(old - new) + jnp.sum(
            jnp.exp2(s - new), axis=0, keepdims=True
        )


def scores_of(scale, text_low, parts):
    rows, tile = text_low.shape[0], 256
    return pl.pallas_call(
        score_kernel,
        grid=(rows // tile,),
        in_specs=[
            pl.BlockSpec(memory_space=pltpu.SMEM),
            pl.BlockSpec((tile, 512), lambda i: (i, 0)),
            *[pl.BlockSpec((256, 512), lambda i: (0, 0)) for _ in range(8)],
        ],
        out_specs=[
            pl.BlockSpec((tile, 2048), lambda i: (i, 0)),
            pl.BlockSpec((2, tile), lambda i: (0, i)),
            pl.BlockSpec((2, 2048), lambda i: (0, 0)),
        ],
        out_shape=[
            jax.ShapeDtypeStruct((rows, 2048), F32),
            jax.ShapeDtypeStruct((2, rows), F32),
            jax.ShapeDtypeStruct((2, 2048), F32),
        ],
        scratch_shapes=[pltpu.VMEM((2048, 512), BF)],
        name="scores",
    )(scale, text_low, *parts)


def grad_kernel(place_ref, scale_ref, s_ref, row_ref, col_ref, *refs):
    parts, (g_ref, share_ref, image) = refs[:8], refs[8:]
    step = pl.program_id(0)
    section = place_ref[0]
    own = place_ref[1] * 2 + place_ref[2]

    @pl.when(step == 0)
    def _():
        assemble(parts, image)

    row_max = to_sublanes(row_ref[0:1, :])
    row_mul = to_sublanes(0.5 / row_ref[1:2, :])
    col_max = col_ref[0:1, :]
    col_mul = 0.5 / col_ref[1:2, :]
    s = s_ref[...]
    g = jnp.exp2(s - row_max) * row_mul + jnp.exp2(s - col_max) * col_mul
    g_ref[...] = g.astype(BF)

    @pl.when(step == own)
    def _():
        for half in range(2):

            @pl.when(section == half)
            def _():
                cut = slice(half * 128, half * 128 + 128)
                r = lax.broadcasted_iota(jnp.int32, (128, 128), 0)
                c = lax.broadcasted_iota(jnp.int32, (128, 128), 1)
                d = s_ref[cut, 0:128]
                d = (
                    jnp.exp2(d - row_max[cut]) * row_mul[cut]
                    + jnp.exp2(d - col_max[:, 0:128]) * col_mul[:, 0:128]
                    - (r == c).astype(F32)
                )
                g_ref[cut, 0:128] = d.astype(BF)

    share = (dot(g_ref[...], image[...]) * scale_ref[0]).astype(BF)
    share_ref[0, section, 0] = share[0:128]
    share_ref[0, 1 - section, 0] = share[128:256]


def score_grads(place, scale, s, row, col, parts):
    rows, tile = s.shape[0], 256
    return pl.pallas_call(
        grad_kernel,
        grid_spec=pltpu.PrefetchScalarGridSpec(
            num_scalar_prefetch=1,
            grid=(rows // tile,),
            in_specs=[
                pl.BlockSpec(memory_space=pltpu.SMEM),
                pl.BlockSpec((tile, 2048), lambda i, p: (i, 0)),
                pl.BlockSpec((2, tile), lambda i, p: (0, i)),
                pl.BlockSpec((2, 2048), lambda i, p: (0, 0)),
                *[pl.BlockSpec((256, 512), lambda i, p: (0, 0)) for _ in range(8)],
            ],
            out_specs=[
                pl.BlockSpec((tile, 2048), lambda i, p: (i, 0)),
                pl.BlockSpec(
                    (1, 2, 1, 128, 512),
                    lambda i, p: ((i % 2) ^ p[2], 0, (i // 2) ^ p[1], 0, 0),
                ),
            ],
            scratch_shapes=[pltpu.VMEM((2048, 512), BF)],
        ),
        out_shape=[
            jax.ShapeDtypeStruct((rows, 2048), BF),
            jax.ShapeDtypeStruct((2, 2, 2, 128, 512), BF),
        ],
        name="score_grads",
    )(place, scale, s, row, col, *parts)


def image_share_kernel(place_ref, scale_ref, g_ref, text_ref, out_ref):
    out_ref[0] = (dot_rows(g_ref[...], text_ref[...]) * scale_ref[0]).astype(BF)


def image_shares(dp_place, scale, g, text_low):
    rows = g.shape[0]

    def target(i, p):
        return (((p[0] - i // 4) & 3) * 4 + ((p[1] - i % 4) & 3), 0, 0)

    return pl.pallas_call(
        image_share_kernel,
        grid_spec=pltpu.PrefetchScalarGridSpec(
            num_scalar_prefetch=1,
            grid=(16,),
            in_specs=[
                pl.BlockSpec(memory_space=pltpu.SMEM),
                pl.BlockSpec((rows, 128), lambda i, p: (0, i)),
                pl.BlockSpec((rows, 512), lambda i, p: (0, 0)),
            ],
            out_specs=pl.BlockSpec((1, 128, 512), target),
        ),
        out_shape=jax.ShapeDtypeStruct((16, 128, 512), BF),
        name="image_shares",
    )(dp_place, scale, g, text_low)


def joined(m, total, axis):
    peak = jnp.max(m, axis=axis, keepdims=True)
    return (
        lax.squeeze(peak, (axis,)),
        jnp.sum(total * jnp.exp2(m - peak), axis=axis),
    )


def slopes(pre):
    sigm = jax.nn.sigmoid(1.702 * pre)
    return sigm, sigm + 1.702 * pre * sigm * (1.0 - sigm)


def feed_kernel(place_ref, pieces_ref, unit_ref, len_ref, h_own_ref, h_far_ref, *refs):
    near, far, outs = refs[:4], refs[4:10], refs[10:]
    top_ref, mid_ref, low_ref = outs
    section = place_ref[0]
    unit = unit_ref[...]
    grad = jnp.sum(pieces_ref[...].astype(F32), axis=0)
    top = unit_backward(unit, len_ref[...], grad).astype(BF)
    top_ref[...] = top
    own_blocks = [(r.at[0], r.at[1]) for r in near]
    far_blocks = [
        (far[0].at[0], far[0].at[1]),
        (far[1].at[0], far[1].at[1]),
        (far[2], far[4]),
        (far[3], far[5]),
    ]

    def layer(g, h_ref, blocks):
        total = g.astype(F32)
        for first, second in blocks:
            _, slope = slopes(dot(h_ref[...], first[...]))
            back = dot_cols(g, second[...])
            total = total + dot_cols((back * slope).astype(BF), first[...])
        return total.astype(BF)

    @pl.when(section == 1)
    def _():
        mid = layer(top, h_own_ref, own_blocks)
        mid_ref[...] = mid
        low_ref[...] = layer(mid, h_far_ref, far_blocks)

    @pl.when(section == 0)
    def _():
        mid = layer(top, h_far_ref, far_blocks)
        mid_ref[...] = mid
        low_ref[...] = layer(mid, h_own_ref, own_blocks)


def feed_back(place, pieces, unit, length, h_own, h_far, near, far):
    vmem = pl.BlockSpec(memory_space=pltpu.VMEM)
    out = jax.ShapeDtypeStruct((128, 512), BF)
    return pl.pallas_call(
        feed_kernel,
        in_specs=[pl.BlockSpec(memory_space=pltpu.SMEM)] + [vmem] * (5 + len(near) + len(far)),
        out_specs=[vmem] * 3,
        out_shape=[out] * 3,
        name="feed_back",
    )(place, pieces, unit, length, h_own, h_far, *near, *far)


def block_row(section, chip, core, k, q):
    return ((chip ^ (k & 1)) * 4 + (core ^ q) * 2 + (section ^ (k >> 1))) * 128


def weight_kernel(place_ref, g0_ref, g1_ref, h_ref, first_ref, second_ref, out_ref, g_scr):
    section, chip, core = place_ref[0], place_ref[1], place_ref[2]
    for q, ref in ((0, g0_ref), (1, g1_ref)):
        for k in range(4):
            at = pl.multiple_of(block_row(section, chip, core, k, q), 128)
            g_scr[pl.ds(at, 128), :] = ref[k]
    pre = dot(h_ref[...], first_ref[...])
    sigm, slope = slopes(pre)
    act = (pre * sigm).astype(BF)
    out_ref[:, 512:1024] = dot_rows(g_scr[...], act).astype(BF)
    back = dot_cols(g_scr[...], second_ref[...])
    out_ref[:, 0:512] = dot_rows(h_ref[...], (back * slope).astype(BF)).astype(BF)


def weight_grads(place, g0, g1, h, first, second):
    vmem = pl.BlockSpec(memory_space=pltpu.VMEM)
    return pl.pallas_call(
        weight_kernel,
        in_specs=[pl.BlockSpec(memory_space=pltpu.SMEM)] + [vmem] * 5,
        out_specs=vmem,
        out_shape=jax.ShapeDtypeStruct((512, 1024), BF),
        scratch_shapes=[pltpu.VMEM((1024, 512), BF)],
        name="weight_grads",
    )(place, g0, g1, h, first, second)


def to_chips(near, far):
    return jnp.stack([near, chip_swap(near, 1), chip_swap(far, 2), chip_swap(far, 3)])


def body(text_feats, image_feats, logit_scale, layer_inputs, w_in, w_out):
    section = lax.axis_index("section")
    dp = lax.axis_index("dp")
    mp = lax.axis_index("mp")
    chip, core = mp // 2, mp % 2
    place = jnp.stack([section, chip, core]).astype(jnp.int32)
    dp_place = jnp.stack([dp // 4, dp % 4]).astype(jnp.int32)
    logit_mult = logit_scale[0]
    own_row = mp * 256 + section * 128

    image_own = lax.dynamic_slice_in_dim(image_feats, section * 128, 128, 0)
    image_unit, image_length = unit_rows(image_own)
    image_low = image_unit.astype(BF)
    c0, c1 = image_low[:64], image_low[64:]
    a0 = jnp.concatenate([c0] + [torus_shift(c0, 0, k) for k in (1, 2, 3)])
    b0 = jnp.concatenate([c1] + [torus_shift(c1, k, 0) for k in (1, 2, 3)])
    parts = [a0] + [torus_shift(a0, k, 0) for k in (1, 2, 3)]
    parts += [b0] + [torus_shift(b0, 0, k) for k in (1, 2, 3)]

    h_own_all = layer_inputs[0]
    first, second = w_in[0], w_out[0]
    packed = jnp.stack([first, second])
    near1 = chip_swap(packed, 1)
    far3 = chip_swap(packed, 3)
    far2_first = chip_swap(far3[0], 1)
    far2_second = chip_swap(near1[1], 3)
    near = [packed, near1, core_swap(packed), core_swap(near1)]
    far = [
        far3, core_swap(far3), far2_first, core_swap(far2_first),
        far2_second, core_swap(far2_second),
    ]
    h_own = lax.dynamic_slice_in_dim(h_own_all, own_row, 128, 0)
    h_far = chip_swap(
        lax.dynamic_slice_in_dim(h_own_all, mp * 256 + (1 - section) * 128, 128, 0), 2
    )

    text_unit, text_length = unit_rows(text_feats)
    text_low = text_unit.astype(BF)
    text_own, text_own_length = unit_rows(
        lax.dynamic_slice_in_dim(text_feats, own_row, 128, 0)
    )

    s, row, col = scores_of(logit_scale, text_low, parts)

    row2 = jnp.stack([row, core_swap(row)])
    row2 = jnp.stack(joined(row2[:, 0], row2[:, 1], 0))
    row4 = jnp.stack([row2] + [chip_swap(row2, k) for k in (1, 2, 3)])
    row = jnp.stack(joined(row4[:, 0], row4[:, 1], 0))
    for axis in (2, 1):
        col = col.reshape(2, 4, 4, 128)
        shifts = [
            jnp.roll(torus_shift(col, *((0, k) if axis == 2 else (k, 0))), k, axis)
            for k in (1, 2, 3)
        ]
        four = jnp.stack([col] + shifts)
        col = jnp.stack(joined(four[:, 0], four[:, 1], 0))
    col = col.reshape(2, 2048)

    g, share = score_grads(place, logit_scale, s, row, col, parts)

    kept = (share[0].astype(F32) + core_swap(share[1]).astype(F32)).astype(BF)
    pieces = jnp.stack(
        [kept[0, 0]] + [chip_swap(kept[k >> 1, k & 1], k) for k in (1, 2, 3)]
    )
    top, mid, low = feed_back(
        place, pieces, text_own, text_own_length, h_own, h_far, near, far
    )

    image_parts = lax.all_to_all(
        image_shares(dp_place, logit_scale, g, text_low), "dp", 0, 0, tiled=True
    )
    image_half = unit_backward(
        image_unit, image_length, image_parts.astype(F32).sum(axis=0)
    ).astype(BF)
    image_other = chip_swap(image_half, 2)
    upper = section == 1
    image_grad = jnp.concatenate(
        [
            jnp.where(upper, image_other, image_half),
            jnp.where(upper, image_half, image_other),
        ]
    )

    g0 = to_chips(jnp.where(upper, top, mid), jnp.where(upper, mid, top))
    g1 = core_swap(g0)
    weights = weight_grads(place, g0, g1, h_own_all, first, second)
    sums = lax.all_to_all(weights.reshape(16, 32, 1024), "dp", 0, 0, tiled=True)
    sums = sums.astype(F32).sum(axis=0)

    left, right = low[:, :256], low[:, 256:]
    i0 = to_chips(jnp.where(upper, right, left), jnp.where(upper, left, right))
    i1 = core_swap(i0)
    input_grad = jnp.zeros((1024, 256), BF)
    for q, blocks in ((0, i0), (1, i1)):
        for k in range(4):
            input_grad = lax.dynamic_update_slice_in_dim(
                input_grad, blocks[k], block_row(section, chip, core, k, q), 0
            )
    return (image_grad, input_grad, sums[None, :, :512], sums[None, :, 512:])


def solution(mesh):
    placed = (
        P("dp", None),
        P(("dp", "mp"), None),
        P(),
        P("section", "dp", None),
        P("section", None, "mp"),
        P("section", "mp", None),
    )
    return jax.shard_map(
        body,
        mesh=mesh,
        in_specs=placed,
        out_specs=(
            P(("dp", "mp"), None),
            P("dp", "section"),
            P("section", "dp", "mp"),
            P("section", "dp", "mp"),
        ),
        check_vma=False,
    )
```

```python
import functools

import jax
import jax.numpy as jnp
from jax import lax
from jax.experimental import pallas as pl
from jax.experimental.pallas import tpu as pltpu
from jax.sharding import PartitionSpec as P


BF = jnp.bfloat16
F32 = jnp.float32
LOG2E = 1.4426950408889634
GROUP = ("section", "mp")


def unit_rows(values):
    wide = values.astype(F32)
    length = jnp.sqrt(jnp.sum(wide * wide, axis=1, keepdims=True) + 1.0)
    return (wide / length, length)


def unit_backward(unit, length, grad_unit):
    return (grad_unit - unit * jnp.sum(unit * grad_unit, axis=1, keepdims=True)) / length


PLANE = ("dp", "mp")


def turn(value, phase, k):
    route = []
    for z in range(4):
        for y in range(4):
            for m in range(4):
                along_y = (m % 2 == 0) == (phase == 0)
                to = z * 4 + (y + k) % 4 if along_y else (z + k) % 4 * 4 + y
                route.append(((z * 4 + y) * 4 + m, to * 4 + m))
    return lax.ppermute(value, PLANE, route)


def chip_swap(value, k):
    return lax.ppermute(value, GROUP, [(i, i ^ (2 * k)) for i in range(8)])


def core_swap(value):
    return lax.ppermute(value, GROUP, [(i, i ^ 1) for i in range(8)])


def dot_rows(a, b):
    return lax.dot_general(a, b, (((0,), (0,)), ((), ())), preferred_element_type=F32)


def dot_cols(a, b):
    return lax.dot_general(a, b, (((1,), (1,)), ((), ())), preferred_element_type=F32)


def dot(a, b):
    return jnp.dot(a, b, preferred_element_type=F32)


def to_lanes(column):
    return jnp.broadcast_to(column, (column.shape[0], 128)).T[0:1, :]


def to_sublanes(row):
    return jnp.broadcast_to(row, (128, row.shape[1])).T[:, 0:1]


def params(megabytes):
    return pltpu.CompilerParams(vmem_limit_bytes=megabytes << 20)


def cost(flops, transcendentals=0):
    return pl.CostEstimate(flops=flops, transcendentals=transcendentals, bytes_accessed=0)


SMEM = pl.BlockSpec(memory_space=pltpu.SMEM)
VMEM = pl.BlockSpec(memory_space=pltpu.VMEM)


def whole(shape):
    return pl.BlockSpec(shape, lambda *_: (0,) * len(shape))


def block_of(section, chip, core, i):
    return (chip ^ (i & 1)) * 4 + (core ^ ((i >> 2) & 1)) * 2 + (section ^ ((i >> 1) & 1))


def image_kernel(place_ref, feats_ref, low_ref, unit_ref, length_ref):
    unit, length = unit_rows(feats_ref[...])
    low_ref[...] = unit.astype(BF)
    unit_ref[...] = unit
    length_ref[...] = length


def image_units(place, feats):
    return pl.pallas_call(
        image_kernel,
        grid_spec=pltpu.PrefetchScalarGridSpec(
            num_scalar_prefetch=1,
            grid=(1,),
            in_specs=[pl.BlockSpec((128, 512), lambda i, p: (p[0], 0))],
            out_specs=[whole((128, 512)), whole((128, 512)), whole((128, 1))],
        ),
        out_shape=[
            jax.ShapeDtypeStruct((128, 512), BF),
            jax.ShapeDtypeStruct((128, 512), F32),
            jax.ShapeDtypeStruct((128, 1), F32),
        ],
        compiler_params=params(8),
        cost_estimate=cost(1 << 20),
        name="image_units",
    )(place, feats)


def text_kernel(place_ref, feats_ref, low_ref, turned_ref, unit_ref, length_ref):
    unit, length = unit_rows(feats_ref[...])
    low_ref[...] = unit.astype(BF)
    turned_ref[...] = unit.T.astype(BF)

    @pl.when(pl.program_id(0) == 0)
    def _():
        unit_ref[...] = unit
        length_ref[...] = length


def text_units(place, feats):
    return pl.pallas_call(
        text_kernel,
        grid_spec=pltpu.PrefetchScalarGridSpec(
            num_scalar_prefetch=1,
            grid=(8,),
            in_specs=[pl.BlockSpec((128, 512), lambda i, p: (block_of(p[0], p[1], p[2], i), 0))],
            out_specs=[
                pl.BlockSpec((128, 512), lambda i, p: (i, 0)),
                pl.BlockSpec((512, 128), lambda i, p: (0, i)),
                whole((128, 512)),
                whole((128, 1)),
            ],
        ),
        out_shape=[
            jax.ShapeDtypeStruct((1024, 512), BF),
            jax.ShapeDtypeStruct((512, 1024), BF),
            jax.ShapeDtypeStruct((128, 512), F32),
            jax.ShapeDtypeStruct((128, 1), F32),
        ],
        compiler_params=params(8),
        cost_estimate=cost(1 << 26),
        name="text_units",
    )(place, feats)


def merged(m0, l0, m1, l1):
    m = jnp.maximum(m0, m1)
    return m, l0 * jnp.exp2(m0 - m) + l1 * jnp.exp2(m1 - m)


def score_kernel(ks, first, scale_ref, text_ref, *refs):
    n = len(ks)
    images, refs = refs[:n], refs[n:]
    if not first:
        (row_in, col_in), refs = refs[:2], refs[2:]
    s_refs, (row_ref, col_ref) = refs[:n], refs[n:]
    step = pl.program_id(0)

    @pl.when(step == 0)
    def _():
        if first:
            col_ref[:, 0:1, :] = jnp.full((16, 1, 128), -1e30, F32)
            col_ref[:, 1:2, :] = jnp.zeros((16, 1, 128), F32)
        else:
            col_ref[...] = col_in[...]

    mult = scale_ref[0] * LOG2E
    peaks = {}
    high = None
    for image, s_ref, k in zip(images, s_refs, ks):
        s = dot_cols(text_ref[...], image[...]) * mult
        s_ref[...] = s
        for j in range(4):
            part = s[:, j * 128 : j * 128 + 128]
            high = part if high is None else jnp.maximum(high, part)
            peaks[k * 4 + j] = jnp.max(part, axis=0, keepdims=True)
    row_max = jnp.max(high, axis=1, keepdims=True)
    total = jnp.zeros((256, 128), F32)
    for s_ref, k in zip(s_refs, ks):
        for j in range(4):
            part = s_ref[:, j * 128 : j * 128 + 128]
            total = total + jnp.exp2(part - row_max)
            b = k * 4 + j
            old = col_ref[b, 0:1, :]
            new = jnp.maximum(old, peaks[b])
            col_ref[b, 1:2, :] = col_ref[b, 1:2, :] * jnp.exp2(old - new) + jnp.sum(
                jnp.exp2(part - new), axis=0, keepdims=True
            )
            col_ref[b, 0:1, :] = new
    row_m = to_lanes(row_max)
    row_l = to_lanes(jnp.sum(total, axis=1, keepdims=True))
    for i in range(2):
        m, l = row_m[:, i * 128 : i * 128 + 128], row_l[:, i * 128 : i * 128 + 128]
        if not first:
            m, l = merged(row_in[i, 0:1, :], row_in[i, 1:2, :], m, l)
        row_ref[i, 0:1, :] = m
        row_ref[i, 1:2, :] = l


def scores_of(scale, text_low, images, ks, before):
    n = len(ks)
    row_spec = pl.BlockSpec((2, 2, 128), lambda i: (i, 0, 0))
    col_spec = whole((16, 2, 128))
    return pl.pallas_call(
        functools.partial(score_kernel, ks, not before),
        grid=(4,),
        in_specs=[SMEM, pl.BlockSpec((256, 512), lambda i: (i, 0))]
        + [whole((512, 512))] * n
        + ([row_spec, col_spec] if before else []),
        out_specs=[pl.BlockSpec((256, 512), lambda i: (i, 0))] * n + [row_spec, col_spec],
        out_shape=[jax.ShapeDtypeStruct((1024, 512), F32)] * n
        + [jax.ShapeDtypeStruct((8, 2, 128), F32), jax.ShapeDtypeStruct((16, 2, 128), F32)],
        compiler_params=params(16),
        cost_estimate=cost(n << 29, n << 20),
        name="scores",
    )(scale, text_low, *images, *before)


def over_four(refs, places):
    peak = refs[0][places[0], 0:1, :]
    for ref, at in zip(refs[1:], places[1:]):
        peak = jnp.maximum(peak, ref[at, 0:1, :])
    total = jnp.zeros_like(peak)
    for ref, at in zip(refs, places):
        total = total + ref[at, 1:2, :] * jnp.exp2(ref[at, 0:1, :] - peak)
    return peak, 0.5 / total


def grad_kernel(base, scale_ref, *refs):
    s_refs, images, rows, cols = refs[:4], refs[4:8], refs[8:12], refs[12:16]
    g_ref, share_ref, row_scr, col_scr = refs[16:]
    step = pl.program_id(0)

    @pl.when(step == 0)
    def _():
        for b in range(16):
            k, j = b // 4, b % 4
            peak, mult = over_four(cols, [(k - i) % 4 * 4 + j for i in range(4)])
            col_scr[b, 0:1, :] = peak
            col_scr[b, 1:2, :] = mult
        for b in range(4):
            at = base * 2 + b
            peak, mult = over_four(rows, [(at & 4) | ((at & 3) ^ i) for i in range(4)])
            row_scr[b, 0:1, :] = peak
            row_scr[b, 1:2, :] = mult

    def column(stat):
        return jnp.concatenate(
            [to_sublanes(row_scr[2 * step + i, stat : stat + 1, :]) for i in range(2)], axis=0
        )

    row_max, row_mul = column(0), column(1)
    share = jnp.zeros((256, 512), F32)
    for k in range(4):
        for j in range(4):
            cut = slice(j * 128, j * 128 + 128)
            s = s_refs[k][:, cut]
            col_max = col_scr[k * 4 + j, 0:1, :]
            col_mul = col_scr[k * 4 + j, 1:2, :]
            g = jnp.exp2(s - row_max) * row_mul + jnp.exp2(s - col_max) * col_mul
            if base == 0 and k == 0 and j == 0:
                r = lax.broadcasted_iota(jnp.int32, (256, 128), 0) + step * 256
                c = lax.broadcasted_iota(jnp.int32, (256, 128), 1)
                g = g - (r == c).astype(F32)
            g_ref[:, k * 512 + j * 128 : k * 512 + j * 128 + 128] = g.astype(BF)
        share = share + dot(g_ref[:, k * 512 : k * 512 + 512], images[k][...])
    share = (share * scale_ref[0]).astype(BF)
    share_ref[0] = share[0:128]
    share_ref[1] = share[128:256]


def score_grads(base, scale, scores, images, rows, cols):
    return pl.pallas_call(
        functools.partial(grad_kernel, base),
        grid=(2,),
        in_specs=[SMEM]
        + [pl.BlockSpec((256, 512), lambda i: (base + i, 0))] * 4
        + [whole((512, 512))] * 4
        + [whole((8, 2, 128))] * 4
        + [whole((16, 2, 128))] * 4,
        out_specs=[
            pl.BlockSpec((256, 2048), lambda i: (i, 0)),
            pl.BlockSpec((2, 128, 512), lambda i: (i, 0, 0)),
        ],
        out_shape=[
            jax.ShapeDtypeStruct((512, 2048), BF),
            jax.ShapeDtypeStruct((4, 128, 512), BF),
        ],
        scratch_shapes=[pltpu.VMEM((4, 2, 128), F32), pltpu.VMEM((16, 2, 128), F32)],
        compiler_params=params(20),
        cost_estimate=cost(1 << 30, 2 << 20),
        name="score_grads",
    )(scale, *scores, *images, *rows, *cols)


def image_share_kernel(place_ref, scale_ref, turned_ref, keep_ref, send_ref, out_ref):
    k = pl.program_id(0)
    core, z, y = place_ref[2], place_ref[3], place_ref[4]
    share = dot(turned_ref[:, :512], keep_ref[...]) + dot(turned_ref[:, 512:], send_ref[...])
    share = (share * scale_ref[0]).astype(BF)
    for j in range(4):
        zr, yr = jnp.where(core == 0, k, j), jnp.where(core == 0, j, k)
        out_ref[((z - zr) & 3) * 4 + ((y - yr) & 3)] = share[:, j * 128 : j * 128 + 128]


def image_shares(place, scale, turned, keep, send):
    return pl.pallas_call(
        image_share_kernel,
        grid_spec=pltpu.PrefetchScalarGridSpec(
            num_scalar_prefetch=1,
            grid=(4,),
            in_specs=[SMEM, whole((512, 1024))]
            + [pl.BlockSpec((512, 512), lambda i, p: (0, i))] * 2,
            out_specs=whole((16, 512, 128)),
        ),
        out_shape=jax.ShapeDtypeStruct((16, 512, 128), BF),
        compiler_params=params(20),
        cost_estimate=cost(1 << 31),
        name="image_shares",
    )(place, scale, turned, keep, send)


def image_end_kernel(parts_ref, unit_ref, length_ref, out_ref):
    grad = jnp.sum(parts_ref[...].astype(F32), axis=0).T
    out_ref[...] = unit_backward(unit_ref[...], length_ref[...], grad).astype(BF)


def image_end(parts, unit, length):
    return pl.pallas_call(
        image_end_kernel,
        in_specs=[VMEM] * 3,
        out_specs=VMEM,
        out_shape=jax.ShapeDtypeStruct((128, 512), BF),
        compiler_params=params(16),
        cost_estimate=cost(1 << 24),
        name="image_end",
    )(parts, unit, length)


def joined(m, total, axis):
    peak = jnp.max(m, axis=axis)
    return jnp.stack(
        [peak, jnp.sum(total * jnp.exp2(m - jnp.expand_dims(peak, axis)), axis=axis)], axis=1
    )


def slopes(pre):
    sigm = jax.nn.sigmoid(1.702 * pre)
    return sigm, sigm + 1.702 * pre * sigm * (1.0 - sigm)


def slope_kernel(h_ref, *refs):
    for i in range(4):
        refs[4][i] = slopes(dot(h_ref[...], refs[i][...]))[1]


def slopes_of(h, firsts):
    return pl.pallas_call(
        slope_kernel,
        in_specs=[VMEM] * 5,
        out_specs=VMEM,
        out_shape=jax.ShapeDtypeStruct((4, 128, 512), F32),
        compiler_params=params(12),
        cost_estimate=cost(1 << 28, 1 << 18),
        name="slopes",
    )(h, *firsts)


def one_layer(g, slope_ref, blocks):
    total = g.astype(F32)
    for i, (first, second) in enumerate(blocks):
        back = dot_cols(g, second[...])
        total = total + dot_cols((back * slope_ref[i]).astype(BF), first[...])
    return total.astype(BF)


def layer_kernel(top, place_ref, *refs):
    if top:
        pieces, (unit_ref, length_ref), refs = refs[:4], refs[4:6], refs[6:]
        grad = sum(p[...].astype(F32) for p in pieces)
        g = unit_backward(unit_ref[...], length_ref[...], grad).astype(BF)
    else:
        g, refs = refs[0][...], refs[1:]
    near_slope, far_slope = refs[:2]
    weights, outs = refs[2:18], refs[18:]
    near = [(weights[i], weights[4 + i]) for i in range(4)]
    far = [(weights[8 + i], weights[12 + i]) for i in range(4)]
    section = place_ref[0]
    on_near = 1 if top else 0

    def finish(out, own):
        if top:
            outs[0][...] = out
            outs[1][...] = g if own else out
            outs[2][...] = out if own else g
        else:
            left, right = out[:, :256], out[:, 256:]
            outs[0][...] = left if own else right
            outs[1][...] = right if own else left

    @pl.when(section == on_near)
    def _():
        finish(one_layer(g, near_slope, near), True)

    @pl.when(section != on_near)
    def _():
        finish(one_layer(g, far_slope, far), False)


def layer_back(top, place, inputs, near_slope, far_slope, weights):
    shapes = [(128, 512)] * 3 if top else [(128, 256)] * 2
    args = [*inputs, near_slope, far_slope, *weights]
    return pl.pallas_call(
        functools.partial(layer_kernel, top),
        in_specs=[SMEM] + [VMEM] * len(args),
        out_specs=[VMEM] * len(shapes),
        out_shape=[jax.ShapeDtypeStruct(s, BF) for s in shapes],
        compiler_params=params(16),
        cost_estimate=cost(1 << 29),
        name="layer_back",
    )(place, *args)


def states_kernel(h_ref, first_ref, act_ref, slope_ref):
    pre = dot(h_ref[...], first_ref[...])
    sigm, slope = slopes(pre)
    act_ref[...] = (pre * sigm).astype(BF)
    slope_ref[...] = slope


def states_of(h, first):
    return pl.pallas_call(
        states_kernel,
        grid=(4,),
        in_specs=[pl.BlockSpec((256, 512), lambda i: (i, 0)), whole((512, 512))],
        out_specs=[pl.BlockSpec((256, 512), lambda i: (i, 0))] * 2,
        out_shape=[
            jax.ShapeDtypeStruct((1024, 512), BF),
            jax.ShapeDtypeStruct((1024, 512), F32),
        ],
        compiler_params=params(12),
        cost_estimate=cost(1 << 29, 1 << 19),
        name="states",
    )(h, first)


def weight_kernel(place_ref, h_ref, act_ref, slope_ref, second_ref, *refs):
    blocks, (other_ref, out_ref, g_scr) = refs[:4], refs[4:]
    place = place_ref[0], place_ref[1], place_ref[2]
    for i in range(8):
        at = pl.multiple_of(block_of(*place, i) * 128, 128)
        g_scr[pl.ds(at, 128), :] = blocks[i][...] if i < 4 else other_ref[i - 4]
    out_ref[:, 512:1024] = dot_rows(g_scr[...], act_ref[...]).astype(BF)
    back = dot_cols(g_scr[...], second_ref[...])
    out_ref[:, 0:512] = dot_rows(h_ref[...], (back * slope_ref[...]).astype(BF)).astype(BF)


def weight_grads(place, h, act, slope, second, blocks, other):
    return pl.pallas_call(
        weight_kernel,
        in_specs=[SMEM] + [VMEM] * 9,
        out_specs=VMEM,
        out_shape=jax.ShapeDtypeStruct((512, 1024), BF),
        scratch_shapes=[pltpu.VMEM((1024, 512), BF)],
        compiler_params=params(20),
        cost_estimate=cost(3 << 29),
        name="weight_grads",
    )(place, h, act, slope, second, *blocks, other)


def input_kernel(place_ref, *refs):
    blocks, (other_ref, out_ref) = refs[:4], refs[4:]
    place = place_ref[0], place_ref[1], place_ref[2]
    for i in range(8):
        at = pl.multiple_of(block_of(*place, i) * 128, 128)
        out_ref[pl.ds(at, 128), :] = blocks[i][...] if i < 4 else other_ref[i - 4]


def input_end(place, blocks, other):
    return pl.pallas_call(
        input_kernel,
        in_specs=[SMEM] + [VMEM] * 5,
        out_specs=VMEM,
        out_shape=jax.ShapeDtypeStruct((1024, 256), BF),
        compiler_params=params(8),
        cost_estimate=cost(1 << 24),
        name="input_end",
    )(place, *blocks, other)


def sum_kernel(parts_ref, first_ref, second_ref):
    total = jnp.sum(parts_ref[...].astype(F32), axis=0)
    first_ref[0] = total[:, :512]
    second_ref[0] = total[:, 512:]


def weight_end(parts):
    return pl.pallas_call(
        sum_kernel,
        in_specs=[VMEM],
        out_specs=[VMEM] * 2,
        out_shape=[jax.ShapeDtypeStruct((1, 32, 512), F32)] * 2,
        compiler_params=params(8),
        cost_estimate=cost(1 << 24),
        name="weight_end",
    )(parts)


def to_chips(near, far):
    return [near, chip_swap(near, 1), chip_swap(far, 2), chip_swap(far, 3)]


def body(text_feats, image_feats, logit_scale, layer_inputs, w_in, w_out):
    section = lax.axis_index("section")
    dp = lax.axis_index("dp")
    mp = lax.axis_index("mp")
    place = jnp.stack([section, mp // 2, mp % 2, dp // 4, dp % 4]).astype(jnp.int32)
    scale = logit_scale

    image_low, image_unit, image_length = image_units(place, image_feats)
    images = [jnp.concatenate([image_low] + [turn(image_low, 0, j) for j in (1, 2, 3)])]
    images += [turn(images[0], 1, k) for k in (1, 2, 3)]

    h = layer_inputs[0]
    first, second = w_in[0], w_out[0]
    near_first, near_second = chip_swap(first, 1), chip_swap(second, 1)
    far_first, far_second = chip_swap(first, 3), chip_swap(second, 3)
    far2_first, far2_second = chip_swap(far_first, 1), chip_swap(near_second, 3)
    near_firsts = [first, near_first, core_swap(first), core_swap(near_first)]
    near_seconds = [second, near_second, core_swap(second), core_swap(near_second)]
    far_firsts = [far_first, far2_first, core_swap(far_first), core_swap(far2_first)]
    far_seconds = [far_second, far2_second, core_swap(far_second), core_swap(far2_second)]
    weights = near_firsts + near_seconds + far_firsts + far_seconds
    h_own = lax.dynamic_slice_in_dim(h, mp * 256 + section * 128, 128, 0)
    h_far = chip_swap(lax.dynamic_slice_in_dim(h, mp * 256 + (1 - section) * 128, 128, 0), 2)

    text_low, text_turned, text_unit, text_length = text_units(place, text_feats)
    act, slope = states_of(h, first)

    s0, *before = scores_of(scale, text_low, images[:1], (0,), ())
    s1, s3, *before = scores_of(scale, text_low, [images[1], images[3]], (1, 3), before)
    s2, row, col = scores_of(scale, text_low, images[2:3], (2,), before)
    scores = [s0, s1, s2, s3]

    shifted = [
        jnp.roll(turn(col, 0, j).reshape(4, 4, 2, 128), j, 1).reshape(16, 2, 128)
        for j in (1, 2, 3)
    ]
    other = core_swap(row)
    other = jnp.concatenate([other[4:], other[:4]])
    pair = jnp.stack([row, other])
    row = joined(pair[:, :, 0], pair[:, :, 1], 0)
    rows = [row] + [chip_swap(row, k) for k in (1, 2, 3)]
    four = jnp.stack([col] + shifted)
    col = joined(four[:, :, 0], four[:, :, 1], 0)
    cols = [col] + [turn(col, 1, k) for k in (1, 2, 3)]

    g_send, share_send = score_grads(2, scale, scores, images, rows, cols)
    received = core_swap(share_send)
    g_keep, share_keep = score_grads(0, scale, scores, images, rows, cols)
    kept = (share_keep.astype(F32) + received.astype(F32)).astype(BF)
    pieces = [kept[0]] + [chip_swap(kept[k], k) for k in (1, 2, 3)]

    near_slope = slopes_of(h_own, near_firsts)
    far_slope = slopes_of(h_far, far_firsts)
    mid, to_near, to_far = layer_back(
        True, place, pieces + [text_unit, text_length], near_slope, far_slope, weights
    )
    grads = to_chips(to_near, to_far)
    half_near, half_far = layer_back(False, place, [mid], near_slope, far_slope, weights)

    image_parts = lax.all_to_all(
        image_shares(place, scale, text_turned, g_keep, g_send), "dp", 0, 0, tiled=True
    )
    image_half = image_end(image_parts, image_unit, image_length)
    image_other = chip_swap(image_half, 2)
    upper = section == 1
    image_grad = jnp.concatenate(
        [
            jnp.where(upper, image_other, image_half),
            jnp.where(upper, image_half, image_other),
        ]
    )

    sums = weight_grads(
        place, h, act, slope, second, grads, core_swap(jnp.stack(grads))
    )
    sums = lax.all_to_all(sums.reshape(16, 32, 1024), "dp", 0, 0, tiled=True)
    first_sum, second_sum = weight_end(sums)

    halves = to_chips(half_near, half_far)
    input_grad = input_end(place, halves, core_swap(jnp.stack(halves)))
    return (image_grad, input_grad, first_sum, second_sum)


def solution(mesh):
    placed = (
        P("dp", None),
        P(("dp", "mp"), None),
        P(),
        P("section", "dp", None),
        P("section", None, "mp"),
        P("section", "mp", None),
    )
    return jax.shard_map(
        body,
        mesh=mesh,
        in_specs=placed,
        out_specs=(
            P(("dp", "mp"), None),
            P("dp", "section"),
            P("section", "dp", "mp"),
            P("section", "dp", "mp"),
        ),
        check_vma=False,
    )
```

```python
import functools

import jax
import jax.numpy as jnp
from jax import lax
from jax.experimental import pallas as pl
from jax.experimental.pallas import tpu as pltpu
from jax.sharding import PartitionSpec as P


BF = jnp.bfloat16
F32 = jnp.float32
LOG2E = 1.4426950408889634
GROUP = ("section", "mp")


def unit_rows(values):
    wide = values.astype(F32)
    length = jnp.sqrt(jnp.sum(wide * wide, axis=1, keepdims=True) + 1.0)
    return (wide / length, length)


def unit_backward(unit, length, grad_unit):
    return (grad_unit - unit * jnp.sum(unit * grad_unit, axis=1, keepdims=True)) / length


PLANE = ("dp", "mp")


def turn(value, phase, k):
    route = []
    for z in range(4):
        for y in range(4):
            for m in range(4):
                along_y = (m % 2 == 0) == (phase == 0)
                to = z * 4 + (y + k) % 4 if along_y else (z + k) % 4 * 4 + y
                route.append(((z * 4 + y) * 4 + m, to * 4 + m))
    return lax.ppermute(value, PLANE, route)


def chip_swap(value, k):
    return lax.ppermute(value, GROUP, [(i, i ^ (2 * k)) for i in range(8)])


def core_swap(value):
    return lax.ppermute(value, GROUP, [(i, i ^ 1) for i in range(8)])


def dot_rows(a, b):
    return lax.dot_general(a, b, (((0,), (0,)), ((), ())), preferred_element_type=F32)


def dot_cols(a, b):
    return lax.dot_general(a, b, (((1,), (1,)), ((), ())), preferred_element_type=F32)


def dot(a, b):
    return jnp.dot(a, b, preferred_element_type=F32)


def to_lanes(column):
    return jnp.broadcast_to(column, (column.shape[0], 128)).T[0:1, :]


def to_sublanes(row):
    return jnp.broadcast_to(row, (128, row.shape[1])).T[:, 0:1]


def params():
    return pltpu.CompilerParams(vmem_limit_bytes=20 << 20)


def cost(flops, transcendentals=0):
    return pl.CostEstimate(flops=flops, transcendentals=transcendentals, bytes_accessed=0)


SMEM = pl.BlockSpec(memory_space=pltpu.SMEM)
VMEM = pl.BlockSpec(memory_space=pltpu.VMEM)


def whole(shape):
    return pl.BlockSpec(shape, lambda *_: (0,) * len(shape))


def block_of(section, chip, core, i):
    return (chip ^ (i & 1)) * 4 + (core ^ ((i >> 2) & 1)) * 2 + (section ^ ((i >> 1) & 1))


def image_kernel(place_ref, feats_ref, low_ref, unit_ref, length_ref):
    unit, length = unit_rows(feats_ref[...])
    low_ref[...] = unit.astype(BF)
    unit_ref[...] = unit
    length_ref[...] = length


def image_units(place, feats):
    return pl.pallas_call(
        image_kernel,
        grid_spec=pltpu.PrefetchScalarGridSpec(
            num_scalar_prefetch=1,
            grid=(1,),
            in_specs=[pl.BlockSpec((128, 512), lambda i, p: (p[0], 0))],
            out_specs=[whole((128, 512)), whole((128, 512)), whole((128, 1))],
        ),
        out_shape=[
            jax.ShapeDtypeStruct((128, 512), BF),
            jax.ShapeDtypeStruct((128, 512), F32),
            jax.ShapeDtypeStruct((128, 1), F32),
        ],
        compiler_params=params(),
        cost_estimate=cost(1 << 20),
        name="image_units",
    )(place, feats)


def text_kernel(place_ref, feats_ref, low_ref, turned_ref, unit_ref, length_ref):
    unit, length = unit_rows(feats_ref[...])
    low_ref[...] = unit.astype(BF)
    turned_ref[...] = unit.T.astype(BF)

    @pl.when(pl.program_id(0) == 0)
    def _():
        unit_ref[...] = unit
        length_ref[...] = length


def text_units(place, feats):
    return pl.pallas_call(
        text_kernel,
        grid_spec=pltpu.PrefetchScalarGridSpec(
            num_scalar_prefetch=1,
            grid=(8,),
            in_specs=[pl.BlockSpec((128, 512), lambda i, p: (block_of(p[0], p[1], p[2], i), 0))],
            out_specs=[
                pl.BlockSpec((128, 512), lambda i, p: (i, 0)),
                pl.BlockSpec((512, 128), lambda i, p: (0, i)),
                whole((128, 512)),
                whole((128, 1)),
            ],
        ),
        out_shape=[
            jax.ShapeDtypeStruct((1024, 512), BF),
            jax.ShapeDtypeStruct((512, 1024), BF),
            jax.ShapeDtypeStruct((128, 512), F32),
            jax.ShapeDtypeStruct((128, 1), F32),
        ],
        compiler_params=params(),
        cost_estimate=cost(1 << 26),
        name="text_units",
    )(place, feats)


def merged(m0, l0, m1, l1):
    m = jnp.maximum(m0, m1)
    return m, l0 * jnp.exp2(m0 - m) + l1 * jnp.exp2(m1 - m)


def score_kernel(ks, first, scale_ref, text_ref, *refs):
    n = len(ks)
    images, refs = refs[:n], refs[n:]
    if not first:
        (row_in, col_in), refs = refs[:2], refs[2:]
    s_refs, (row_ref, col_ref) = refs[:n], refs[n:]
    step = pl.program_id(0)

    @pl.when(step == 0)
    def _():
        if first:
            col_ref[:, 0:1, :] = jnp.full((16, 1, 128), -1e30, F32)
            col_ref[:, 1:2, :] = jnp.zeros((16, 1, 128), F32)
        else:
            col_ref[...] = col_in[...]

    mult = scale_ref[0] * LOG2E
    peaks = {}
    high = None
    for image, s_ref, k in zip(images, s_refs, ks):
        s = dot_cols(text_ref[...], image[...]) * mult
        s_ref[...] = s
        for j in range(4):
            part = s[:, j * 128 : j * 128 + 128]
            high = part if high is None else jnp.maximum(high, part)
            peaks[k * 4 + j] = jnp.max(part, axis=0, keepdims=True)
    row_max = jnp.max(high, axis=1, keepdims=True)
    total = jnp.zeros((256, 128), F32)
    for s_ref, k in zip(s_refs, ks):
        for j in range(4):
            part = s_ref[:, j * 128 : j * 128 + 128]
            total = total + jnp.exp2(part - row_max)
            b = k * 4 + j
            old = col_ref[b, 0:1, :]
            new = jnp.maximum(old, peaks[b])
            col_ref[b, 1:2, :] = col_ref[b, 1:2, :] * jnp.exp2(old - new) + jnp.sum(
                jnp.exp2(part - new), axis=0, keepdims=True
            )
            col_ref[b, 0:1, :] = new
    row_m = to_lanes(row_max)
    row_l = to_lanes(jnp.sum(total, axis=1, keepdims=True))
    for i in range(2):
        m, l = row_m[:, i * 128 : i * 128 + 128], row_l[:, i * 128 : i * 128 + 128]
        if not first:
            m, l = merged(row_in[i, 0:1, :], row_in[i, 1:2, :], m, l)
        row_ref[i, 0:1, :] = m
        row_ref[i, 1:2, :] = l


def scores_of(scale, text_low, images, ks, before):
    n = len(ks)
    row_spec = pl.BlockSpec((2, 2, 128), lambda i: (i, 0, 0))
    col_spec = whole((16, 2, 128))
    return pl.pallas_call(
        functools.partial(score_kernel, ks, not before),
        grid=(4,),
        in_specs=[SMEM, pl.BlockSpec((256, 512), lambda i: (i, 0))]
        + [whole((512, 512))] * n
        + ([row_spec, col_spec] if before else []),
        out_specs=[pl.BlockSpec((256, 512), lambda i: (i, 0))] * n + [row_spec, col_spec],
        out_shape=[jax.ShapeDtypeStruct((1024, 512), F32)] * n
        + [jax.ShapeDtypeStruct((8, 2, 128), F32), jax.ShapeDtypeStruct((16, 2, 128), F32)],
        compiler_params=params(),
        cost_estimate=cost(n << 29, n << 20),
        name="scores",
    )(scale, text_low, *images, *before)


def over_four(refs, places):
    peak = refs[0][places[0], 0:1, :]
    for ref, at in zip(refs[1:], places[1:]):
        peak = jnp.maximum(peak, ref[at, 0:1, :])
    total = jnp.zeros_like(peak)
    for ref, at in zip(refs, places):
        total = total + ref[at, 1:2, :] * jnp.exp2(ref[at, 0:1, :] - peak)
    return peak, total


def grad_kernel(base, scale_ref, *refs):
    s_refs, images, rows, cols = refs[:4], refs[4:8], refs[8:12], refs[12:16]
    g_ref, share_ref, row_scr, col_scr = refs[16:]
    step = pl.program_id(0)

    @pl.when(step == 0)
    def _():
        for b in range(16):
            k, j = b // 4, b % 4
            peak, total = over_four(cols, [(k - i) % 4 * 4 + j for i in range(4)])
            col_scr[b, 0:1, :] = peak
            col_scr[b, 1:2, :] = 0.5 / total
        for b in range(4):
            at = base * 2 + b
            peak, total = over_four(rows, [(at & 4) | ((at & 3) ^ i) for i in range(4)])
            row_scr[b, 0:1, :] = peak
            row_scr[b, 1:2, :] = 0.5 / total

    def column(stat):
        return jnp.concatenate(
            [to_sublanes(row_scr[2 * step + i, stat : stat + 1, :]) for i in range(2)], axis=0
        )

    row_max, row_mul = column(0), column(1)
    share = jnp.zeros((256, 512), F32)
    for k in range(4):
        for j in range(4):
            cut = slice(j * 128, j * 128 + 128)
            s = s_refs[k][:, cut]
            col_max = col_scr[k * 4 + j, 0:1, :]
            col_mul = col_scr[k * 4 + j, 1:2, :]
            g = jnp.exp2(s - row_max) * row_mul + jnp.exp2(s - col_max) * col_mul
            if base == 0 and k == 0 and j == 0:
                r = lax.broadcasted_iota(jnp.int32, (256, 128), 0) + step * 256
                c = lax.broadcasted_iota(jnp.int32, (256, 128), 1)
                g = g - (r == c).astype(F32)
            g_ref[:, k * 512 + j * 128 : k * 512 + j * 128 + 128] = g.astype(BF)
        share = share + dot(g_ref[:, k * 512 : k * 512 + 512], images[k][...])
    share = (share * scale_ref[0]).astype(BF)
    share_ref[0] = share[0:128]
    share_ref[1] = share[128:256]


def score_grads(base, scale, scores, images, rows, cols):
    return pl.pallas_call(
        functools.partial(grad_kernel, base),
        grid=(2,),
        in_specs=[SMEM]
        + [pl.BlockSpec((256, 512), lambda i: (base + i, 0))] * 4
        + [whole((512, 512))] * 4
        + [whole((8, 2, 128))] * 4
        + [whole((16, 2, 128))] * 4,
        out_specs=[
            pl.BlockSpec((256, 2048), lambda i: (i, 0)),
            pl.BlockSpec((2, 128, 512), lambda i: (i, 0, 0)),
        ],
        out_shape=[
            jax.ShapeDtypeStruct((512, 2048), BF),
            jax.ShapeDtypeStruct((4, 128, 512), BF),
        ],
        scratch_shapes=[pltpu.VMEM((4, 2, 128), F32), pltpu.VMEM((16, 2, 128), F32)],
        compiler_params=params(),
        cost_estimate=cost(1 << 30, 2 << 20),
        name="score_grads",
    )(scale, *scores, *images, *rows, *cols)


def image_share_kernel(scale_ref, turned_ref, keep_ref, send_ref, *outs):
    step = pl.program_id(0)
    share = dot(turned_ref[:, :512], keep_ref[...]) + dot(turned_ref[:, 512:], send_ref[...])
    share = (share * scale_ref[0]).astype(BF)
    for k in range(4):

        @pl.when(step == k)
        def _():
            for j in range(4):
                outs[k][j] = share[:, j * 128 : j * 128 + 128]


def image_shares(scale, turned, keep, send):
    return pl.pallas_call(
        image_share_kernel,
        grid=(4,),
        in_specs=[SMEM, whole((512, 1024))] + [pl.BlockSpec((512, 512), lambda i: (0, i))] * 2,
        out_specs=[whole((4, 512, 128))] * 4,
        out_shape=[jax.ShapeDtypeStruct((4, 512, 128), BF)] * 4,
        compiler_params=params(),
        cost_estimate=cost(1 << 31),
        name="image_shares",
    )(scale, turned, keep, send)


def split_sum_kernel(*refs):
    parts, outs = refs[:-4], refs[-4:]
    for i in range(4):
        outs[i][...] = sum(p[i].astype(F32) for p in parts).astype(BF)


def split_sum(parts):
    return pl.pallas_call(
        split_sum_kernel,
        in_specs=[VMEM] * len(parts),
        out_specs=[VMEM] * 4,
        out_shape=[jax.ShapeDtypeStruct(parts[0].shape[1:], BF)] * 4,
        compiler_params=params(),
        cost_estimate=cost(1 << 24),
        name="split_sum",
    )(*parts)


def image_end_kernel(unit_ref, length_ref, *refs):
    grad = sum(p[...].astype(F32) for p in refs[:4]).T
    refs[4][...] = unit_backward(unit_ref[...], length_ref[...], grad).astype(BF)


def image_end(parts, unit, length):
    return pl.pallas_call(
        image_end_kernel,
        in_specs=[VMEM] * 6,
        out_specs=VMEM,
        out_shape=jax.ShapeDtypeStruct((128, 512), BF),
        compiler_params=params(),
        cost_estimate=cost(1 << 24),
        name="image_end",
    )(unit, length, *parts)


def join_kernel(place_ref, own_ref, other_ref, out_ref):
    section = place_ref[0]
    out_ref[pl.ds(pl.multiple_of(section * 128, 128), 128), :] = own_ref[...]
    out_ref[pl.ds(pl.multiple_of((1 - section) * 128, 128), 128), :] = other_ref[...]


def image_join(place, own, other):
    return pl.pallas_call(
        join_kernel,
        in_specs=[SMEM, VMEM, VMEM],
        out_specs=VMEM,
        out_shape=jax.ShapeDtypeStruct((256, 512), BF),
        compiler_params=params(),
        cost_estimate=cost(1 << 22),
        name="image_join",
    )(place, own, other)


def pick_kernel(place_ref, h_ref, own_ref, far_ref):
    @pl.when(pl.program_id(0) == 0)
    def _():
        own_ref[...] = h_ref[...]

    @pl.when(pl.program_id(0) == 1)
    def _():
        far_ref[...] = h_ref[...]


def pick_rows(place, h):
    return pl.pallas_call(
        pick_kernel,
        grid_spec=pltpu.PrefetchScalarGridSpec(
            num_scalar_prefetch=1,
            grid=(2,),
            in_specs=[
                pl.BlockSpec((128, 512), lambda i, p: (p[1] * 4 + p[2] * 2 + (p[0] ^ i), 0))
            ],
            out_specs=[whole((128, 512))] * 2,
        ),
        out_shape=[jax.ShapeDtypeStruct((128, 512), BF)] * 2,
        compiler_params=params(),
        cost_estimate=cost(1 << 22),
        name="pick_rows",
    )(place, h)


def row_pair_kernel(own_ref, other_ref, out_ref):
    for b in range(8):
        m, l = merged(
            own_ref[b, 0:1, :], own_ref[b, 1:2, :],
            other_ref[b ^ 4, 0:1, :], other_ref[b ^ 4, 1:2, :],
        )
        out_ref[b, 0:1, :] = m
        out_ref[b, 1:2, :] = l


def row_pair(own, other):
    return pl.pallas_call(
        row_pair_kernel,
        in_specs=[VMEM] * 2,
        out_specs=VMEM,
        out_shape=jax.ShapeDtypeStruct((8, 2, 128), F32),
        compiler_params=params(),
        cost_estimate=cost(1 << 22),
        name="row_pair",
    )(own, other)


def col_line_kernel(*refs):
    out_ref = refs[4]
    for b in range(16):
        k, j = b // 4, b % 4
        peak, total = over_four(refs[:4], [k * 4 + (j - i) % 4 for i in range(4)])
        out_ref[b, 0:1, :] = peak
        out_ref[b, 1:2, :] = total


def col_line(cols):
    return pl.pallas_call(
        col_line_kernel,
        in_specs=[VMEM] * 4,
        out_specs=VMEM,
        out_shape=jax.ShapeDtypeStruct((16, 2, 128), F32),
        compiler_params=params(),
        cost_estimate=cost(1 << 22),
        name="col_line",
    )(*cols)


def slopes(pre):
    sigm = jax.nn.sigmoid(1.702 * pre)
    return sigm, sigm + 1.702 * pre * sigm * (1.0 - sigm)


def slope_kernel(h_ref, *refs):
    for i in range(4):
        refs[4][i] = slopes(dot(h_ref[...], refs[i][...]))[1]


def slopes_of(h, firsts):
    return pl.pallas_call(
        slope_kernel,
        in_specs=[VMEM] * 5,
        out_specs=VMEM,
        out_shape=jax.ShapeDtypeStruct((4, 128, 512), F32),
        compiler_params=params(),
        cost_estimate=cost(1 << 28, 1 << 18),
        name="slopes",
    )(h, *firsts)


def one_layer(g, slope_ref, blocks):
    total = g.astype(F32)
    for i, (first, second) in enumerate(blocks):
        back = dot_cols(g, second[...])
        total = total + dot_cols((back * slope_ref[i]).astype(BF), first[...])
    return total.astype(BF)


def layer_kernel(top, place_ref, *refs):
    if top:
        pieces, (unit_ref, length_ref), refs = refs[:4], refs[4:6], refs[6:]
        grad = sum(p[...].astype(F32) for p in pieces)
        g = unit_backward(unit_ref[...], length_ref[...], grad).astype(BF)
    else:
        g, refs = refs[0][...], refs[1:]
    near_slope, far_slope = refs[:2]
    weights, outs = refs[2:18], refs[18:]
    near = [(weights[i], weights[4 + i]) for i in range(4)]
    far = [(weights[8 + i], weights[12 + i]) for i in range(4)]
    section = place_ref[0]
    on_near = 1 if top else 0

    def finish(out, own):
        if top:
            outs[0][...] = out
            outs[1][...] = g if own else out
            outs[2][...] = out if own else g
        else:
            left, right = out[:, :256], out[:, 256:]
            outs[0][...] = left if own else right
            outs[1][...] = right if own else left

    @pl.when(section == on_near)
    def _():
        finish(one_layer(g, near_slope, near), True)

    @pl.when(section != on_near)
    def _():
        finish(one_layer(g, far_slope, far), False)


def layer_back(top, place, inputs, near_slope, far_slope, weights):
    shapes = [(128, 512)] * 3 if top else [(128, 256)] * 2
    args = [*inputs, near_slope, far_slope, *weights]
    return pl.pallas_call(
        functools.partial(layer_kernel, top),
        in_specs=[SMEM] + [VMEM] * len(args),
        out_specs=[VMEM] * len(shapes),
        out_shape=[jax.ShapeDtypeStruct(s, BF) for s in shapes],
        compiler_params=params(),
        cost_estimate=cost(1 << 29),
        name="layer_back",
    )(place, *args)


def states_kernel(h_ref, first_ref, act_ref, slope_ref):
    pre = dot(h_ref[...], first_ref[...])
    sigm, slope = slopes(pre)
    act_ref[...] = (pre * sigm).astype(BF)
    slope_ref[...] = slope


def states_of(h, first):
    return pl.pallas_call(
        states_kernel,
        grid=(4,),
        in_specs=[pl.BlockSpec((256, 512), lambda i: (i, 0)), whole((512, 512))],
        out_specs=[pl.BlockSpec((256, 512), lambda i: (i, 0))] * 2,
        out_shape=[
            jax.ShapeDtypeStruct((1024, 512), BF),
            jax.ShapeDtypeStruct((1024, 512), F32),
        ],
        compiler_params=params(),
        cost_estimate=cost(1 << 29, 1 << 19),
        name="states",
    )(h, first)


def weight_kernel(place_ref, h_ref, act_ref, slope_ref, second_ref, *refs):
    blocks, other_ref, outs, (g_scr, w_scr) = refs[:4], refs[4], refs[5:9], refs[9:]
    place = place_ref[0], place_ref[1], place_ref[2]
    for i in range(8):
        at = pl.multiple_of(block_of(*place, i) * 128, 128)
        g_scr[pl.ds(at, 128), :] = blocks[i][...] if i < 4 else other_ref[i - 4]
    w_scr[:, 512:1024] = dot_rows(g_scr[...], act_ref[...]).astype(BF)
    back = dot_cols(g_scr[...], second_ref[...])
    w_scr[:, 0:512] = dot_rows(h_ref[...], (back * slope_ref[...]).astype(BF)).astype(BF)
    core, z, y = place_ref[2], place_ref[3], place_ref[4]
    for k in range(4):
        for j in range(4):
            zr, yr = jnp.where(core == 0, k, j), jnp.where(core == 0, j, k)
            at = pl.multiple_of((((z - zr) & 3) * 4 + ((y - yr) & 3)) * 32, 32)
            outs[k][j] = w_scr[pl.ds(at, 32), :]


def weight_grads(place, h, act, slope, second, blocks, other):
    return pl.pallas_call(
        weight_kernel,
        in_specs=[SMEM] + [VMEM] * 9,
        out_specs=[VMEM] * 4,
        out_shape=[jax.ShapeDtypeStruct((4, 32, 1024), BF)] * 4,
        scratch_shapes=[pltpu.VMEM((1024, 512), BF), pltpu.VMEM((512, 1024), BF)],
        compiler_params=params(),
        cost_estimate=cost(3 << 29),
        name="weight_grads",
    )(place, h, act, slope, second, *blocks, other)


def input_kernel(place_ref, *refs):
    out_ref = refs[4]
    place = place_ref[0], place_ref[1], place_ref[2]
    for i in range(8):
        at = pl.multiple_of(block_of(*place, i) * 128, 128)
        out_ref[pl.ds(at, 128), :] = refs[(i >> 2) * 2 + (i & 1)][(i >> 1) & 1]


def input_end(place, blocks):
    return pl.pallas_call(
        input_kernel,
        in_specs=[SMEM] + [VMEM] * 4,
        out_specs=VMEM,
        out_shape=jax.ShapeDtypeStruct((1024, 256), BF),
        compiler_params=params(),
        cost_estimate=cost(1 << 24),
        name="input_end",
    )(place, *blocks)


def sum_kernel(*refs):
    total = sum(p[...].astype(F32) for p in refs[:4])
    refs[4][0] = total[:, :512]
    refs[5][0] = total[:, 512:]


def weight_end(parts):
    return pl.pallas_call(
        sum_kernel,
        in_specs=[VMEM] * 4,
        out_specs=[VMEM] * 2,
        out_shape=[jax.ShapeDtypeStruct((1, 32, 512), F32)] * 2,
        compiler_params=params(),
        cost_estimate=cost(1 << 24),
        name="weight_end",
    )(*parts)


ROUTE = (1, 3, 2)


def spread(f, values):
    got = {i: f(values[i], i) for i in ROUTE}
    return [values[0]] + [got[i] for i in (1, 2, 3)]


def along(phase, sign=1):
    return lambda value, k: turn(value, phase, sign * k)


def steps(text_feats, image_feats, logit_scale, layer_inputs, w_in, w_out):
    section = lax.axis_index("section")
    dp = lax.axis_index("dp")
    mp = lax.axis_index("mp")
    place = jnp.stack([section, mp >> 1, mp & 1, dp >> 2, dp & 3]).astype(jnp.int32)
    scale = logit_scale

    image_feats = pltpu.with_memory_space_constraint(image_feats, pltpu.HBM)
    image_low, image_unit, image_length = image_units(place, image_feats)
    line = jnp.concatenate(spread(along(0), [image_low] * 4))
    images = spread(along(1), [line] * 4)

    h = layer_inputs[0]
    first, second = w_in[0], w_out[0]
    near_first, near_second = chip_swap(first, 1), chip_swap(second, 1)
    far_first, far_second = chip_swap(first, 3), chip_swap(second, 3)
    far2_first = chip_swap(far_first, 1)
    far2_second = chip_swap(near_second, 3)
    h_own, h_send = pick_rows(place, h)
    h_far = chip_swap(h_send, 2)
    near_firsts = [first, near_first, core_swap(first), core_swap(near_first)]
    near_seconds = [second, near_second, core_swap(second), core_swap(near_second)]
    far_firsts = [far_first, far2_first, core_swap(far_first), core_swap(far2_first)]
    far_seconds = [
        far_second, far2_second,
        core_swap(far_second), core_swap(far2_second),
    ]
    weights = near_firsts + near_seconds + far_firsts + far_seconds

    text_low, text_turned, text_unit, text_length = text_units(place, text_feats)
    act, slope = states_of(h, first)

    s0, *before = scores_of(scale, text_low, images[:1], (0,), ())
    s1, s3, *before = scores_of(scale, text_low, [images[1], images[3]], (1, 3), before)
    s2, row, col = scores_of(scale, text_low, images[2:3], (2,), before)
    scores = [s0, s1, s2, s3]

    row = row_pair(row, core_swap(row))
    col = col_line(spread(along(0), [col] * 4))
    cols = spread(along(1), [col] * 4)
    rows = spread(chip_swap, [row] * 4)

    g_send, share_send = score_grads(2, scale, scores, images, rows, cols)
    received = core_swap(share_send)
    g_keep, share_keep = score_grads(0, scale, scores, images, rows, cols)
    kept = split_sum([share_keep, received])
    pieces = spread(chip_swap, kept)

    near_slope = slopes_of(h_own, near_firsts)
    far_slope = slopes_of(h_far, far_firsts)
    mid, to_near, to_far = layer_back(
        True, place, pieces + [text_unit, text_length],
        near_slope, far_slope, weights,
    )
    grads = spread(chip_swap, [to_near, to_near, to_far, to_far])
    half_near, half_far = layer_back(False, place, [mid], near_slope, far_slope, weights)

    other = core_swap(jnp.stack(grads))
    sums = weight_grads(place, h, act, slope, second, grads, other)
    sums = split_sum(spread(along(1, -1), sums))
    first_sum, second_sum = weight_end(spread(along(0, -1), sums))

    shares = image_shares(scale, text_turned, g_keep, g_send)
    parts = split_sum(spread(along(1, -1), shares))
    image_half = image_end(spread(along(0, -1), parts), image_unit, image_length)
    image_grad = image_join(place, image_half, chip_swap(image_half, 2))

    even = jnp.stack([half_near, chip_swap(half_far, 2)])
    odd = chip_swap(even, 1)
    input_grad = input_end(place, [even, odd, core_swap(even), core_swap(odd)])
    return (image_grad, input_grad, first_sum, second_sum)


def solution(mesh):
    placed = (
        P("dp", None),
        P(("dp", "mp"), None),
        P(),
        P("section", "dp", None),
        P("section", None, "mp"),
        P("section", "mp", None),
    )
    return jax.shard_map(
        steps,
        mesh=mesh,
        in_specs=placed,
        out_specs=(
            P(("dp", "mp"), None),
            P("dp", "section"),
            P("section", "dp", "mp"),
            P("section", "dp", "mp"),
        ),
        check_vma=False,
    )
```
